256 devices in a mesh: section: 2 (over core), rep: 8 (over z_lo, x), tp: 16 (over z_hi, y).
Axes of the slice: x: 4, y: 4, z: 8 (z_hi: 4, z_lo: 2; z = z_hi * 2 + z_lo), core: 2. Of those that a mesh axis runs over, the one named last changes fastest.
Arguments:
- states: bfloat16 [2, 8, 256, 8192], P('section', 'rep', None, 'tp'), may hold values from -6 to 6
- q_weight: bfloat16 [8192, 4096], P(None, 'tp'), may hold values from -0.0625 to 0.0625
- kv_weight: bfloat16 [8192, 1024], P('tp'), may hold values from -0.0625 to 0.0625
- o_weight: bfloat16 [4096, 8192], P(None, 'tp'), may hold values from -0.09375 to 0.09375
- store_keys: bfloat16 [2, 8, 4096, 512], P('section', 'rep', 'tp'), may hold values from -170 to 170
- store_values: bfloat16 [2, 8, 4096, 512], P('section', 'rep', 'tp'), may hold values from -48 to 48
- prefix_len: int32 [8], replicated, may hold values from 1024 to 4096
- cache_len: int32 [8, 4], P('rep'), may hold values from 128 to 1024
- parents: int32 [8, 4, 64], P('rep'), may hold values from -1 to 62, as said below
Outputs:
- attn_out: bfloat16 [2, 8, 256, 8192], P('section', 'rep', None, 'tp')
The draws below stay inside these ranges and needn't reach their ends.
Inputs may be any that keep to these rules, and one draw needn't show every extreme that they name: `parents`: each node's parent is an earlier node of the same tree; only node 0 has -1.
All inputs are finite; a program needn't handle non-finite values.
Results may differ from the reference program's by a relative error of at most 0.0065.
The reference program's roundings to bfloat16 on the way count: a program that leaves them out, or rounds other values in their place, can miss the bound.
Values may be sent and summed in bfloat16 or wider, within the bound.
A program may use at most 64 MiB of HBM per device.

```python
import jax
import jax.numpy as jnp
from jax import lax

D = 8192
QH = 32
KVH = 4
HD = 128
SEQS = 4
NODES = 64
CACHE = 1024
ROWS = 256
CTX = 4096
QW = 4096
KW = 512
N_SECTION = 2
N_REP = 8
N_TP = 16


def draw_store_keys(key, part):
    full_shape = (N_SECTION, N_REP, CTX, KVH * HD)
    return jnp.clip(2.0 * jax.random.normal(key, full_shape, jnp.float32), -12.0, 12.0).astype(jnp.bfloat16)


def draw_parents(key, part):
    node_ids = jnp.arange(NODES, dtype=jnp.int32)
    offsets = jax.random.randint(key, (N_REP, SEQS, NODES), 1, 5, dtype=jnp.int32)
    return jnp.where(node_ids == 0, -1, jnp.maximum(node_ids - offsets, 0)).astype(jnp.int32)


def with_ends(entries, key, least, top_value):
    index_at = [jax.random.randint(jax.random.fold_in(key, axis), (), 0, length) for axis, length in enumerate(entries.shape)]
    longest = entries.shape.index(max(entries.shape))
    neighbour = index_at[:longest] + [(index_at[longest] + 1) % entries.shape[longest]] + index_at[longest + 1:]
    return entries.at[tuple(index_at)].set(least).at[tuple(neighbour)].set(top_value)


def levels(rng, dims, shards, low, largest):
    factor_of = 1.0
    for axis_at, blocks in shards:
        draws = jax.random.uniform(jax.random.fold_in(jax.random.fold_in(rng, 6), axis_at), (blocks,), jnp.float32, low / len(shards), largest / len(shards))
        factor_of = factor_of * jnp.repeat(jnp.exp(draws), dims[axis_at] // blocks).reshape((-1,) + (1,) * (len(dims) - 1 - axis_at))
    return factor_of


def gaussian(stream_key, extent, width, reach, shards=(), held_as=jnp.bfloat16):
    level = levels(stream_key, extent, shards, -0.22, 0.18) if shards else 1.0
    entries = jax.random.normal(stream_key, extent, jnp.float32) * width * level
    return jnp.minimum(jnp.maximum(entries, -reach), reach).astype(held_as)


def setup_inputs(seed: int = 0) -> dict:
    streams_of = jax.random.split(jax.random.key(seed), 10)
    return {
        "states": gaussian(streams_of[0], (N_SECTION, N_REP, ROWS, D), 1.0, 6.0, ((0, 2), (1, 8), (3, 16))),
        "q_weight": gaussian(streams_of[1], (D, QW), D ** -0.5, 0.0625, ((1, 16),)),
        "kv_weight": gaussian(streams_of[2], (D, 2 * KW), D ** -0.5, 0.0625, ((0, 16),)),
        "o_weight": gaussian(streams_of[3], (QW, D), QW ** -0.5, 0.09375, ((1, 16),)),
        "store_keys": draw_store_keys(jax.random.fold_in(streams_of[9], 71), 0),
        "store_values": gaussian(streams_of[5], (N_SECTION, N_REP, CTX, KW), 8.0, 48.0, ((0, 2), (1, 8), (2, 16))),
        "prefix_len": with_ends(jax.random.randint(streams_of[6], (N_REP,), CTX // 4, CTX + 1), jax.random.fold_in(streams_of[6], 1), CTX // 4, CTX).astype(jnp.int32),
        "cache_len": with_ends(jax.random.randint(streams_of[7], (N_REP, SEQS), CACHE // 8, CACHE + 1), jax.random.fold_in(streams_of[7], 1), CACHE // 8, CACHE).astype(jnp.int32),
        "parents": draw_parents(jax.random.fold_in(streams_of[9], 71), 0),
    }


ROPE_BASE = 500000.0
MASKED_SCORE = -1e30


def rotate(vectors, positions):
    head_size = vectors.shape[-1]
    half_width = head_size // 2
    exponent = jnp.arange(half_width, dtype=jnp.float32) * (-2.0 / head_size)
    frequency = jnp.exp(exponent * jnp.log(jnp.float32(ROPE_BASE)))
    angles = positions.astype(jnp.float32)[:, None] * frequency[None, :]
    cosine = jnp.cos(angles)[:, None, :]
    sine_of = jnp.sin(angles)[:, None, :]
    front_half = vectors[..., :half_width]
    back_half = vectors[..., half_width:]
    return jnp.concatenate([front_half * cosine - back_half * sine_of, back_half * cosine + front_half * sine_of], axis=-1)


def closure(parents):
    node_count = parents.shape[-1]
    node_ids = jnp.arange(node_count, dtype=jnp.int32)
    reached = (parents[:, :, None] == node_ids[None, None, :]).astype(jnp.float32)
    reached = reached + jnp.eye(node_count, dtype=jnp.float32)[None]
    for level_index in range(max(1, (node_count - 1).bit_length())):
        reached = jnp.minimum(jnp.einsum("sij,sjk->sik", reached, reached, precision=lax.Precision.HIGHEST), 1.0)
    return reached


def block_partial(queries, all_keys, all_values, visible):
    row_count = queries.shape[0]
    kv_heads = all_keys.shape[1] // HD
    group_size = queries.shape[1] // all_keys.shape[1]
    row_tops = []
    row_totals = []
    mixtures = []
    for kv_head in range(kv_heads):
        query_block = queries[:, kv_head * group_size * HD:(kv_head + 1) * group_size * HD].reshape(row_count * group_size, HD)
        key_block = all_keys[:, kv_head * HD:(kv_head + 1) * HD]
        value_block = all_values[:, kv_head * HD:(kv_head + 1) * HD]
        scores = lax.dot_general(query_block, key_block, (((1,), (1,)), ((), ())), preferred_element_type=jnp.float32)
        scores = scores.reshape(row_count, group_size, -1) * (HD ** -0.5)
        scores = jnp.where(visible[:, None, :], scores, MASKED_SCORE)
        row_top = jnp.max(scores, axis=-1)
        weights = jnp.where(visible[:, None, :], jnp.exp(scores - row_top[..., None]), 0.0)
        row_total = jnp.sum(weights, axis=-1)
        mixed_rows = jnp.dot(weights.astype(jnp.bfloat16).reshape(row_count * group_size, -1), value_block, preferred_element_type=jnp.float32)
        mixed_rows = mixed_rows.reshape(row_count, group_size, HD) / jnp.maximum(row_total, 1.0)[..., None]
        row_tops.append(row_top)
        row_totals.append(row_total)
        mixtures.append(mixed_rows.reshape(row_count, group_size * HD).astype(jnp.bfloat16))
    return jnp.concatenate(row_tops, axis=1), jnp.concatenate(row_totals, axis=1), jnp.concatenate(mixtures, axis=1)


def finish(tops, totals, parts):
    piece_count, row_count, head_count = tops.shape
    best = jnp.max(tops, axis=0)
    factor = jnp.exp(tops - best[None]) * totals
    denominator = jnp.sum(factor, axis=0)
    numerator = jnp.sum(parts.astype(jnp.float32).reshape(piece_count, row_count, head_count, HD) * factor[..., None], axis=0)
    return (numerator / denominator[..., None]).reshape(row_count, head_count * HD).astype(jnp.bfloat16)


def attend(queries, blocks):
    tops = []
    totals = []
    parts = []
    for keys, values, visible in blocks:
        top, total, part = block_partial(queries, keys, values, visible)
        tops.append(top)
        totals.append(total)
        parts.append(part)
    return finish(jnp.stack(tops), jnp.stack(totals), jnp.stack(parts))


def reference(states, q_weight, kv_weight, o_weight, store_keys, store_values, prefix_len, cache_len, parents):
    row_count = SEQS * NODES
    kv_width = KVH * HD
    store_rows = CTX // N_TP
    block_rows = row_count // N_TP
    row_ids = jnp.arange(row_count, dtype=jnp.int32)
    seq_of = row_ids // NODES
    store_pos = jnp.arange(CTX, dtype=jnp.int32)
    eye_seq = (jnp.arange(SEQS)[:, None] == jnp.arange(SEQS)[None, :]).astype(jnp.float32)

    def project(inputs, positions):
        new_queries = jnp.dot(inputs, q_weight, preferred_element_type=jnp.float32).reshape(row_count, QH, HD)
        new_queries = rotate(new_queries, positions).reshape(row_count, QH * HD).astype(jnp.bfloat16)
        kv_proj = jnp.dot(inputs, kv_weight, preferred_element_type=jnp.float32)
        new_keys = rotate(kv_proj[:, :kv_width].reshape(row_count, KVH, HD), positions).reshape(row_count, kv_width).astype(jnp.bfloat16)
        new_values = kv_proj[:, kv_width:].astype(jnp.bfloat16)
        return new_queries, new_keys, new_values

    prefill_outs = []
    tail_key_list = []
    tail_value_list = []
    for replica in range(N_REP):
        positions = prefix_len[replica] + row_ids
        new_queries, new_keys, new_values = project(states[0, replica], positions)
        blocks = []
        for block in range(N_TP):
            store_lo = block * store_rows
            new_lo = block * block_rows
            store_mask = jnp.broadcast_to(store_pos[None, store_lo:store_lo + store_rows] < prefix_len[replica], (row_count, store_rows))
            causal = row_ids[None, new_lo:new_lo + block_rows] <= row_ids[:, None]
            visible = jnp.concatenate([store_mask, causal], axis=1)
            keys = jnp.concatenate([store_keys[0, replica, store_lo:store_lo + store_rows], new_keys[new_lo:new_lo + block_rows]], axis=0)
            values = jnp.concatenate([store_values[0, replica, store_lo:store_lo + store_rows], new_values[new_lo:new_lo + block_rows]], axis=0)
            blocks.append((keys, values, visible))
        attended = attend(new_queries, blocks)
        prefill_outs.append(jnp.dot(attended, o_weight, preferred_element_type=jnp.float32).astype(jnp.bfloat16))
        tail_key_list.append(new_keys)
        tail_value_list.append(new_values)

    decode_outs = []
    for replica in range(N_REP):
        source_rep = replica
        reached = closure(parents[replica])
        depths = (jnp.sum(reached, axis=-1).astype(jnp.int32) - 1).reshape(row_count)
        seq_lengths = jnp.broadcast_to(cache_len[replica][:, None], (SEQS, NODES)).reshape(row_count)
        base_pos = jnp.where(seq_of == 0, prefix_len[source_rep] + row_count, seq_lengths)
        positions = base_pos + depths
        new_queries, new_keys, new_values = project(states[1, replica], positions)
        tree_mask = (eye_seq[:, None, :, None] * reached[:, :, None, :]).reshape(row_count, row_count) > 0.5
        source_keys = tail_key_list[source_rep]
        source_values = tail_value_list[source_rep]
        blocks = []
        for block in range(N_TP):
            store_lo = block * store_rows
            new_lo = block * block_rows
            block_pos = store_pos[store_lo:store_lo + store_rows]
            store_mask = ((block_pos[None, :] // CACHE) == seq_of[:, None]) & ((block_pos[None, :] % CACHE) < seq_lengths[:, None])
            tail_mask = jnp.broadcast_to((seq_of == 0)[:, None], (row_count, block_rows))
            visible = jnp.concatenate([store_mask, tree_mask[:, new_lo:new_lo + block_rows], tail_mask], axis=1)
            keys = jnp.concatenate([store_keys[1, replica, store_lo:store_lo + store_rows], new_keys[new_lo:new_lo + block_rows], source_keys[new_lo:new_lo + block_rows]], axis=0)
            values = jnp.concatenate([store_values[1, replica, store_lo:store_lo + store_rows], new_values[new_lo:new_lo + block_rows], source_values[new_lo:new_lo + block_rows]], axis=0)
            blocks.append((keys, values, visible))
        attended = attend(new_queries, blocks)
        decode_outs.append(jnp.dot(attended, o_weight, preferred_element_type=jnp.float32).astype(jnp.bfloat16))
    return jnp.stack([jnp.stack(prefill_outs), jnp.stack(decode_outs)])
```

```python
import functools

import jax
import jax.numpy as jnp
import numpy as np
from jax import lax
from jax.experimental import pallas as pl
from jax.experimental.pallas import tpu as pltpu
from jax.sharding import PartitionSpec as P

MESH = pl.DeviceIdType.MESH
HD = 128
ROWS = 256
NODES = 64
ROPE_BASE = 500000.0
MASKED_SCORE = -1e30
F32 = jnp.float32
BF16 = jnp.bfloat16


def slot_of(dz, dy):
    return dy * 4 + dz


class Exchange:
    def __init__(self, view, send_sems, recv_sems, at, pending):
        self.view, self.send_sems, self.recv_sems = view, send_sems, recv_sems
        self.at, self.pending, self.used = at, pending, 0

    def send(self, src, dst_slot, half, dz, dy):
        copy = pltpu.make_async_remote_copy(
            src_ref=src,
            dst_ref=self.view(dst_slot, half),
            send_sem=self.send_sems.at[self.used],
            recv_sem=self.recv_sems.at[dst_slot, half],
            device_id={"tp": self.at(dz, dy)},
            device_id_type=MESH,
        )
        self.used += 1
        copy.start()
        self.pending.append(copy)

    def arrived(self, dz, dy, half):
        slot = slot_of(dz, dy)
        view = self.view(slot, half)
        pltpu.make_async_remote_copy(
            src_ref=view,
            dst_ref=view,
            send_sem=self.send_sems.at[0],
            recv_sem=self.recv_sems.at[slot, half],
            device_id={"tp": self.at(1, 0)},
            device_id_type=MESH,
        ).wait_recv()

    def own_z(self, half):
        self.send(self.view(0, half), slot_of(1, 0), half, 1, 0)
        self.send(self.view(0, half), slot_of(3, 0), half, -1, 0)

    def relay_z(self, half):
        src = self.view(slot_of(1 if half == 0 else 3, 0), half)
        self.send(src, slot_of(2, 0), half, 1 if half == 0 else -1, 0)

    def along_y(self, dz, half):
        src = self.view(slot_of(dz, 0), half)
        self.send(src, slot_of(dz, 1), half, 0, 1)
        self.send(src, slot_of(dz, 3), half, 0, -1)

    def relay_y(self, dz, half):
        src = self.view(slot_of(dz, 1 if half == 0 else 3), half)
        self.send(src, slot_of(dz, 2), half, 0, 1 if half == 0 else -1)

    def near_y(self, dz):
        self.arrived(dz, 1, 0)
        self.relay_y(dz, 0)
        self.arrived(dz, 3, 1)
        self.relay_y(dz, 1)
        self.arrived(dz, 3, 0)
        self.arrived(dz, 1, 1)

    def far_y(self, dz):
        self.arrived(dz, 2, 0)
        self.arrived(dz, 2, 1)


def dot(a, b, dims=((1,), (0,))):
    return lax.dot_general(a, b, (dims, ((), ())), preferred_element_type=F32)


def iota(shape, dim):
    return lax.broadcasted_iota(jnp.int32, shape, dim)


def kernel(
    prefix_ref, cache_ref, parents_ref, freq_ref, x_hbm, wq_hbm, wkv_hbm, wo_hbm, sk_hbm, sv_hbm,
    out_ref,
    xg, wq, wkv, wo, kvps, kvpr, kg, vg, relay, nkv, tail, qacc, qh, closed, cos_ref, sin_ref,
    top_ref, total_ref, mix_ref, ag, oacc,
    local, x_send, x_recv, k_send, k_recv, r_recv, p_send, p_recv, n_send, n_recv, t_sem, a_send, a_recv,
):
    tp = lax.axis_index("tp")
    sec = lax.axis_index("section")
    rep = lax.axis_index("rep")
    z, y = tp // 4, tp % 4

    def at(dz, dy):
        return ((z + dz + 4) % 4) * 4 + (y + dy + 4) % 4

    def head_cols(dz):
        return pl.ds(pl.multiple_of(((z + dz + 4) % 4) * HD, HD), HD)

    def load(src, dst, index):
        copy = pltpu.make_async_copy(src, dst, local.at[index])
        copy.start()
        return copy

    x_in = load(x_hbm, xg.at[0], 0)
    wkv_in = load(wkv_hbm, wkv, 1)
    wq_in = load(wq_hbm, wq, 2)
    k_in = load(sk_hbm.at[:, head_cols(0)], kg.at[0], 3)
    v_in = load(sv_hbm.at[:, head_cols(0)], vg.at[0], 4)
    wo_in = load(wo_hbm, wo, 5)

    barrier = pltpu.get_barrier_semaphore()
    peers = [(dz, dy) for dy in range(4) for dz in range(4) if (dz, dy) != (0, 0)]
    for dz, dy in peers:
        pl.semaphore_signal(barrier, inc=1, device_id={"tp": at(dz, dy)}, device_id_type=MESH)
    pl.semaphore_signal(barrier, inc=1, device_id={"section": 1 - sec}, device_id_type=MESH)
    pl.semaphore_wait(barrier, 16)

    pending = []
    xs = Exchange(lambda s, h: xg.at[s, h], x_send, x_recv, at, pending)
    ks = Exchange(lambda s, h: (kg if h == 0 else vg).at[s], k_send, k_recv, at, pending)
    ats = Exchange(lambda s, h: ag.at[s, h], a_send, a_recv, at, pending)

    x_in.wait()
    for half in range(2):
        xs.own_z(half)
        xs.along_y(0, half)

    wkv_in.wait()
    own_x = xg[0].reshape(ROWS, -1)
    for head in range(4):
        for kind in range(2):
            cols = pl.ds(kind * 512 + head * HD, HD)
            part = dot(own_x, wkv[:, cols]).astype(BF16)
            kvps[:, head, :, pl.ds(kind * HD, HD)] = part.reshape(4, NODES, HD)

    for dz in (1, -1):
        ks.send(sk_hbm.at[:, head_cols(dz)], slot_of(dz % 4, 0), 0, dz, 0)
        ks.send(sv_hbm.at[:, head_cols(dz)], slot_of(dz % 4, 0), 1, dz, 0)

    def to_relay(src, half, dz):
        copy = pltpu.make_async_remote_copy(
            src_ref=src,
            dst_ref=relay.at[half],
            send_sem=k_send.at[ks.used],
            recv_sem=r_recv.at[half],
            device_id={"tp": at(dz, 0)},
            device_id_type=MESH,
        )
        ks.used += 1
        copy.start()
        pending.append(copy)
        return copy

    relays = [to_relay(sk_hbm.at[:, head_cols(2)], 0, 1), to_relay(sv_hbm.at[:, head_cols(2)], 1, -1)]

    parts_in = []
    for n, (dz, dy) in enumerate(peers):
        copy = pltpu.make_async_remote_copy(
            src_ref=kvps.at[(y + dy) % 4, (z + dz) % 4],
            dst_ref=kvpr.at[slot_of(dz, dy)],
            send_sem=p_send.at[n],
            recv_sem=p_recv.at[slot_of(dz, dy)],
            device_id={"tp": at(dz, dy)},
            device_id_type=MESH,
        )
        copy.start()
        pending.append(copy)
        parts_in.append(copy)

    row = iota((ROWS, ROWS), 0)
    col = iota((ROWS, ROWS), 1)
    spread = (iota((NODES, ROWS), 1) % NODES == iota((NODES, ROWS), 0)).astype(BF16)
    parents = dot(parents_ref[...].astype(F32).astype(BF16), spread)
    own_seq = iota((4, ROWS), 1) // NODES == iota((4, ROWS), 0)
    parent = jnp.sum(jnp.where(own_seq, parents, 0.0), axis=0, keepdims=True)
    node = iota((1, ROWS), 1)
    parent_at = jnp.where(parent < 0.0, -1.0, parent + (node // NODES * NODES).astype(F32))
    child = (row.astype(F32) == parent_at).astype(BF16)
    eye = (row == col).astype(BF16)
    closed[...] = (dot(child, eye, ((0,), (0,))) + eye.astype(F32)).astype(BF16)

    def square(level, carry):
        closed[...] = jnp.minimum(dot(closed[...], closed[...]), 1.0).astype(BF16)
        return carry

    lax.fori_loop(0, 6, square, 0)
    depths = dot(closed[...], jnp.ones((ROWS, HD), BF16)).astype(jnp.int32) - 1
    wide_row = iota((ROWS, HD), 0)
    seq = wide_row // NODES
    prefix = prefix_ref[rep]
    base = jnp.full((ROWS, HD), prefix + ROWS, jnp.int32)
    for s in range(1, 4):
        base = jnp.where(seq == s, cache_ref[0, s], base)
    positions = sec * (base + depths) + (1 - sec) * (prefix + wide_row)
    angles = positions.astype(F32) * freq_ref[...]
    cos_ref[...] = jnp.cos(angles)
    lane = iota((ROWS, HD), 1)
    sin_ref[...] = jnp.where(lane < HD // 2, -jnp.sin(angles), jnp.sin(angles))

    def rotate(v, cosine, sine):
        return v * cosine + pltpu.roll(v, HD // 2, 1) * sine

    wq_in.wait()

    def project(dz, dy, first=False):
        source = pl.multiple_of(at(-dz, -dy) * 512, 512)
        part = dot(xg[slot_of(dz, dy)].reshape(ROWS, -1), wq[pl.ds(source, 512), :])
        qacc[...] = part if first else qacc[...] + part

    xs.near_y(0)
    project(0, 0, True)
    xs.arrived(1, 0, 0)
    xs.relay_z(0)
    xs.along_y(1, 0)
    xs.arrived(3, 0, 0)
    xs.along_y(3, 0)
    xs.arrived(3, 0, 1)
    xs.relay_z(1)
    xs.along_y(3, 1)
    xs.arrived(1, 0, 1)
    xs.along_y(1, 1)
    project(0, 1)
    project(0, 3)
    project(1, 0)
    project(3, 0)
    xs.far_y(0)
    project(0, 2)
    for half in range(2):
        relays[half].wait_recv()
        ks.send(relay.at[half], slot_of(2, 0), half, 1 if half == 0 else -1, 0)
    xs.near_y(1)
    xs.near_y(3)
    for half in range(2):
        xs.arrived(2, 0, half)
        xs.along_y(2, half)
    project(1, 1)
    project(1, 3)
    project(3, 1)
    project(3, 3)
    project(2, 0)

    k_in.wait()
    v_in.wait()
    for dz in (0, 1, 3):
        for half in range(2):
            if dz:
                ks.arrived(dz, 0, half)
            ks.along_y(dz, half)

    for copy in parts_in:
        copy.wait_recv()
    fresh = kvps[y, z].astype(F32)
    for dz, dy in peers:
        fresh = fresh + kvpr[slot_of(dz, dy)].astype(F32)
    rows = pl.ds(pl.multiple_of(y * NODES, NODES), NODES)
    fresh_keys = rotate(fresh[:, :HD], cos_ref[rows, :], sin_ref[rows, :])
    nkv[0, y] = fresh_keys.astype(BF16)
    nkv[1, y] = fresh[:, HD:].astype(BF16)

    xs.far_y(1)
    xs.far_y(3)
    project(1, 2)
    project(3, 2)

    news = []
    for dy in range(1, 4):
        copy = pltpu.make_async_remote_copy(
            src_ref=nkv.at[:, y],
            dst_ref=nkv.at[:, y],
            send_sem=n_send.at[dy],
            recv_sem=n_recv.at[dy],
            device_id={"tp": at(0, dy)},
            device_id_type=MESH,
        )
        copy.start()
        pending.append(copy)

    xs.near_y(2)
    project(2, 1)
    project(2, 3)
    for half in range(2):
        ks.arrived(2, 0, half)
        ks.along_y(2, half)
    for dy in range(1, 4):
        piece = nkv.at[:, (y + 4 - dy) % 4]
        pltpu.make_async_remote_copy(
            src_ref=piece,
            dst_ref=piece,
            send_sem=n_send.at[dy],
            recv_sem=n_recv.at[dy],
            device_id={"tp": at(0, dy)},
            device_id_type=MESH,
        ).wait_recv()
    swap = pltpu.make_async_remote_copy(
        src_ref=nkv,
        dst_ref=tail,
        send_sem=t_sem.at[0],
        recv_sem=t_sem.at[1],
        device_id={"section": 1 - sec},
        device_id_type=MESH,
    )
    swap.start()
    pending.append(swap)
    xs.far_y(2)
    project(2, 2)
    for head in range(2):
        qh[head] = rotate(qacc[:, head * HD : (head + 1) * HD], cos_ref[...], sin_ref[...]).astype(BF16)

    seq_wide = row // NODES

    def attend(pieces, first=False):
        def one_head(head, carry):
            queries = qh[head]
            scores = []
            for keys, _, visible in pieces:
                scores.append(jnp.where(visible(), dot(queries, keys(), ((1,), (1,))) * HD**-0.5, MASKED_SCORE))
            best = functools.reduce(jnp.maximum, scores)
            best = jnp.max(best, axis=1, keepdims=True)
            if not first:
                before = top_ref[head][:, :1]
                best = jnp.maximum(best, before)
                fade = jnp.exp(before - best)
            total = 0.0
            mix = 0.0
            for score, (_, values, _) in zip(scores, pieces):
                weights = jnp.exp(score - best)
                total = total + weights
                mix = mix + dot(weights.astype(BF16), values())
            total = jnp.sum(total, axis=1, keepdims=True)
            if not first:
                total = total + total_ref[head][:, :1] * fade
                mix = mix + mix_ref[head] * fade
            top_ref[head] = jnp.broadcast_to(best, (ROWS, HD))
            total_ref[head] = jnp.broadcast_to(total, (ROWS, HD))
            mix_ref[head] = mix
            return carry

        lax.fori_loop(0, 2, one_head, 0)

    def new_visible():
        reached = (closed[...].astype(F32) > 0.5).astype(jnp.int32)
        return sec * reached + (1 - sec) * (col <= row).astype(jnp.int32) > 0

    def tail_visible():
        return sec * (seq_wide == 0).astype(jnp.int32) > 0

    def stored(dz, dy):
        slot = slot_of(dz, dy)
        from_z, from_y = (z - dz + 4) % 4, (y - dy + 4) % 4

        def visible():
            in_prompt = prefix - (from_z * 4 + from_y) * ROWS
            in_cache = cache_ref[0, from_z] - from_y * ROWS
            mine = (seq_wide == from_z).astype(jnp.int32)
            return col < (1 - sec) * in_prompt + sec * in_cache * mine

        return (lambda: kg[slot], lambda: vg[slot], visible)

    attend([(lambda: nkv[0].reshape(ROWS, HD), lambda: nkv[1].reshape(ROWS, HD), new_visible)], True)
    for dz in (0, 1, 3, 2):
        ks.near_y(dz)
    attend([stored(dz, 0) for dz in range(4)])
    swap.wait_recv()
    attend([(lambda: tail[0].reshape(ROWS, HD), lambda: tail[1].reshape(ROWS, HD), tail_visible)])
    attend([stored(dz, 1) for dz in range(4)])
    attend([stored(dz, 3) for dz in range(4)])
    for dz in range(4):
        ks.far_y(dz)
    attend([stored(dz, 2) for dz in range(4)])
    for head in range(2):
        done = (mix_ref[head] / total_ref[head]).astype(BF16)
        ag[0, :, :, head * HD : (head + 1) * HD] = done.reshape(2, ROWS // 2, HD)

    for half in range(2):
        ats.own_z(half)
        ats.along_y(0, half)
    wo_in.wait()

    def finish(dz, dy, first=False):
        source = pl.multiple_of(at(-dz, -dy) * 256, 256)
        part = dot(ag[slot_of(dz, dy)].reshape(ROWS, -1), wo[pl.ds(source, 256), :])
        oacc[...] = part if first else oacc[...] + part

    finish(0, 0, True)
    ats.near_y(0)
    ats.arrived(1, 0, 0)
    ats.relay_z(0)
    ats.along_y(1, 0)
    ats.arrived(3, 0, 0)
    ats.along_y(3, 0)
    ats.arrived(3, 0, 1)
    ats.relay_z(1)
    ats.along_y(3, 1)
    ats.arrived(1, 0, 1)
    ats.along_y(1, 1)
    finish(0, 1)
    finish(0, 3)
    finish(1, 0)
    finish(3, 0)
    ats.far_y(0)
    finish(0, 2)
    for half in range(2):
        ats.arrived(2, 0, half)
        ats.along_y(2, half)
    ats.near_y(1)
    ats.near_y(3)
    finish(2, 0)
    finish(1, 1)
    finish(1, 3)
    finish(3, 1)
    finish(3, 3)
    ats.near_y(2)
    finish(2, 1)
    finish(2, 3)
    ats.far_y(1)
    finish(1, 2)
    ats.far_y(3)
    finish(3, 2)
    ats.far_y(2)
    finish(2, 2)
    out_ref[...] = oacc[...].astype(BF16)
    for copy in pending:
        copy.wait_send()


def per_device(
    states, q_weight, kv_weight, o_weight, store_keys, store_values, prefix_len, cache_len, parents
):
    exponent = np.arange(HD, dtype=np.float32) % (HD // 2) * np.float32(-2.0 / HD)
    frequency = np.exp(exponent * np.log(np.float32(ROPE_BASE))).astype(np.float32)
    x = states[0, 0].reshape(2, ROWS // 2, -1)
    any_space = pl.BlockSpec(memory_space=pl.ANY)
    in_vmem = pl.BlockSpec(memory_space=pltpu.VMEM)
    in_smem = pl.BlockSpec(memory_space=pltpu.SMEM)
    dma = pltpu.SemaphoreType.DMA
    out = pl.pallas_call(
        kernel,
        out_shape=jax.ShapeDtypeStruct((ROWS, o_weight.shape[1]), BF16),
        in_specs=[in_smem, in_smem, in_vmem, in_vmem] + [any_space] * 6,
        out_specs=in_vmem,
        scratch_shapes=[
            pltpu.VMEM((16, 2, ROWS // 2, 512), BF16),
            pltpu.VMEM(q_weight.shape, BF16),
            pltpu.VMEM(kv_weight.shape, BF16),
            pltpu.VMEM(o_weight.shape, BF16),
            pltpu.VMEM((4, 4, NODES, 2 * HD), BF16),
            pltpu.VMEM((16, NODES, 2 * HD), BF16),
            pltpu.VMEM((16, ROWS, HD), BF16),
            pltpu.VMEM((16, ROWS, HD), BF16),
            pltpu.VMEM((2, ROWS, HD), BF16),
            pltpu.VMEM((2, 4, NODES, HD), BF16),
            pltpu.VMEM((2, 4, NODES, HD), BF16),
            pltpu.VMEM((ROWS, 2 * HD), F32),
            pltpu.VMEM((2, ROWS, HD), BF16),
            pltpu.VMEM((ROWS, ROWS), BF16),
            pltpu.VMEM((ROWS, HD), F32),
            pltpu.VMEM((ROWS, HD), F32),
            pltpu.VMEM((2, ROWS, HD), F32),
            pltpu.VMEM((2, ROWS, HD), F32),
            pltpu.VMEM((2, ROWS, HD), F32),
            pltpu.VMEM((16, 2, ROWS // 2, 2 * HD), BF16),
            pltpu.VMEM((ROWS, o_weight.shape[1]), F32),
            dma((6,)),
            dma((32,)),
            dma((16, 2)),
            dma((36,)),
            dma((16, 2)),
            dma((2,)),
            dma((16,)),
            dma((16,)),
            dma((4,)),
            dma((4,)),
            dma((2,)),
            dma((32,)),
            dma((16, 2)),
        ],
        compiler_params=pltpu.CompilerParams(
            collective_id=0, has_side_effects=True, vmem_limit_bytes=56 * 2**20
        ),
    )(
        prefix_len, cache_len, parents[0], jnp.asarray(frequency)[None], x, q_weight, kv_weight, o_weight,
        store_keys[0, 0], store_values[0, 0],
    )
    return out[None, None]


def solution(mesh):
    return jax.shard_map(
        per_device,
        mesh=mesh,
        in_specs=(
            P("section", "rep", None, "tp"),
            P(None, "tp"),
            P("tp", None),
            P(None, "tp"),
            P("section", "rep", "tp", None),
            P("section", "rep", "tp", None),
            P(),
            P("rep", None),
            P("rep", None, None),
        ),
        out_specs=P("section", "rep", None, "tp"),
        check_vma=False,
    )
```

```python
import functools

import jax
import jax.numpy as jnp
import numpy as np
from jax import lax
from jax.experimental import pallas as pl
from jax.experimental.pallas import tpu as pltpu
from jax.sharding import PartitionSpec as P

MESH = pl.DeviceIdType.MESH
HD = 128
ROWS = 256
NODES = 64
ROPE_BASE = 500000.0
MASKED_SCORE = -1e30
F32 = jnp.float32
BF16 = jnp.bfloat16


def slot_of(dz, dy):
    return dy * 4 + dz


class Links:
    def __init__(self, send_sems):
        self.send_sems, self.started = send_sems, []

    def send(self, src, dst, recv_sem, device):
        copy = pltpu.make_async_remote_copy(
            src_ref=src,
            dst_ref=dst,
            send_sem=self.send_sems.at[len(self.started)],
            recv_sem=recv_sem,
            device_id=device,
            device_id_type=MESH,
        )
        copy.start()
        self.started.append(copy)

    def arrived(self, view, recv_sem, device):
        pltpu.make_async_remote_copy(
            src_ref=view,
            dst_ref=view,
            send_sem=self.send_sems.at[0],
            recv_sem=recv_sem,
            device_id=device,
            device_id_type=MESH,
        ).wait_recv()

    def finish(self):
        for copy in self.started:
            copy.wait_send()


class Exchange:
    def __init__(self, links, view, recv_sems, at):
        self.links, self.view, self.recv_sems, self.at = links, view, recv_sems, at

    def send(self, src, dst_slot, half, dz, dy):
        self.links.send(
            src, self.view(dst_slot, half), self.recv_sems.at[dst_slot, half], {"tp": self.at(dz, dy)}
        )

    def arrived(self, dz, dy, half):
        slot = slot_of(dz, dy)
        self.links.arrived(self.view(slot, half), self.recv_sems.at[slot, half], {"tp": self.at(1, 0)})

    def own_z(self, half):
        self.send(self.view(0, half), slot_of(1, 0), half, 1, 0)
        self.send(self.view(0, half), slot_of(3, 0), half, -1, 0)

    def relay_z(self, half):
        src = self.view(slot_of(1 if half == 0 else 3, 0), half)
        self.send(src, slot_of(2, 0), half, 1 if half == 0 else -1, 0)

    def along_y(self, dz, half):
        src = self.view(slot_of(dz, 0), half)
        self.send(src, slot_of(dz, 1), half, 0, 1)
        self.send(src, slot_of(dz, 3), half, 0, -1)

    def relay_y(self, dz, half):
        src = self.view(slot_of(dz, 1 if half == 0 else 3), half)
        self.send(src, slot_of(dz, 2), half, 0, 1 if half == 0 else -1)

    def near_y(self, dz):
        self.arrived(dz, 1, 0)
        self.relay_y(dz, 0)
        self.arrived(dz, 3, 1)
        self.relay_y(dz, 1)
        self.arrived(dz, 3, 0)
        self.arrived(dz, 1, 1)

    def far_y(self, dz):
        self.arrived(dz, 2, 0)
        self.arrived(dz, 2, 1)


def dot(a, b, dims=((1,), (0,))):
    return lax.dot_general(a, b, (dims, ((), ())), preferred_element_type=F32)


def iota(shape, dim):
    return lax.broadcasted_iota(jnp.int32, shape, dim)


def kernel(
    prefix_ref, cache_ref, parents_ref, freq_ref, x_hbm, wq_hbm, wkv_hbm, wo_hbm, sk_hbm, sv_hbm,
    out_ref,
    xg, wl, wg, wkv, wo, kvps, kvpr, kvqs, kvqr, kg, vg, relay, nkv, tail, qacc, qs, qr, qh,
    closed, cos_ref, sin_ref, top_ref, total_ref, mix_ref, ag, oacc,
    local, send_sems, x_recv, k_recv, r_recv, p_recv, u_recv, n_recv, t_recv, a_recv,
    f_recv, g_recv, w_recv, q_recv,
):
    tp = lax.axis_index("tp")
    sec = lax.axis_index("section")
    rep = lax.axis_index("rep")
    z, y = tp // 4, tp % 4
    lane_x = rep % 4
    twin = {"section": 1 - sec}

    def at(dz, dy):
        return ((z + dz + 4) % 4) * 4 + (y + dy + 4) % 4

    def beside(dx):
        return {"rep": rep - lane_x + (lane_x + dx + 4) % 4}

    def head_cols(dz):
        return pl.ds(pl.multiple_of(((z + dz + 4) % 4) * HD, HD), HD)

    def load(src, dst, index):
        copy = pltpu.make_async_copy(src, dst, local.at[index])
        copy.start()
        return copy

    barrier = pltpu.get_barrier_semaphore()
    for dz, dy in ((1, 0), (2, 0), (3, 0), (0, 1), (0, 2), (0, 3)):
        pl.semaphore_signal(barrier, inc=1, device_id={"tp": at(dz, dy)}, device_id_type=MESH)
    for device in (beside(1), beside(-1), twin):
        pl.semaphore_signal(barrier, inc=1, device_id=device, device_id_type=MESH)

    x_in = load(x_hbm, xg.at[0], 0)
    wkv_in = load(wkv_hbm, wkv, 1)
    k_in = load(sk_hbm.at[:, head_cols(0)], kg.at[0], 2)
    v_in = load(sv_hbm.at[:, head_cols(0)], vg.at[0], 3)
    wl_in = [
        load(wq_hbm.at[pl.ds(pl.multiple_of((n * 4 + y) * 512, 512), 512)], wl.at[n], 4 + n) for n in range(4)
    ]
    wo_in = load(wo_hbm, wo, 8)

    x_in.wait()
    wkv_in.wait()
    own_x = xg[0].reshape(ROWS, -1)
    for head in range(4):
        for kind in range(2):
            cols = pl.ds(kind * 512 + head * HD, HD)
            part = dot(own_x, wkv[:, cols]).astype(BF16)
            kvps[:, head, :, pl.ds(kind * HD, HD)] = part.reshape(4, NODES, HD)

    row = iota((ROWS, ROWS), 0)
    col = iota((ROWS, ROWS), 1)
    spread = (iota((NODES, ROWS), 1) % NODES == iota((NODES, ROWS), 0)).astype(BF16)
    parents = dot(parents_ref[...].astype(F32).astype(BF16), spread)
    own_seq = iota((4, ROWS), 1) // NODES == iota((4, ROWS), 0)
    parent = jnp.sum(jnp.where(own_seq, parents, 0.0), axis=0, keepdims=True)
    node = iota((1, ROWS), 1)
    parent_at = jnp.where(parent < 0.0, -1.0, parent + (node // NODES * NODES).astype(F32))
    child = (row.astype(F32) == parent_at).astype(BF16)
    eye = (row == col).astype(BF16)
    closed[...] = (dot(child, eye, ((0,), (0,))) + eye.astype(F32)).astype(BF16)

    def square(level, carry):
        closed[...] = jnp.minimum(dot(closed[...], closed[...]), 1.0).astype(BF16)
        return carry

    lax.fori_loop(0, 6, square, 0)
    depths = dot(closed[...], jnp.ones((ROWS, HD), BF16)).astype(jnp.int32) - 1
    wide_row = iota((ROWS, HD), 0)
    seq = wide_row // NODES
    prefix = prefix_ref[rep]
    base = jnp.full((ROWS, HD), prefix + ROWS, jnp.int32)
    for s in range(1, 4):
        base = jnp.where(seq == s, cache_ref[0, s], base)
    positions = sec * (base + depths) + (1 - sec) * (prefix + wide_row)
    angles = positions.astype(F32) * freq_ref[...]
    cos_ref[...] = jnp.cos(angles)
    lane = iota((ROWS, HD), 1)
    sin_ref[...] = jnp.where(lane < HD // 2, -jnp.sin(angles), jnp.sin(angles))

    def rotate(v, cosine, sine):
        return v * cosine + pltpu.roll(v, HD // 2, 1) * sine

    k_in.wait()
    v_in.wait()
    for copy in wl_in:
        copy.wait()
    wo_in.wait()
    pl.semaphore_wait(barrier, 9)

    links = Links(send_sems)
    xs = Exchange(links, lambda s, h: xg.at[s, h], x_recv, at)
    ks = Exchange(links, lambda s, h: (kg if h == 0 else vg).at[s], k_recv, at)
    ats = Exchange(links, lambda s, h: ag.at[s, h], a_recv, at)

    for dy in (1, 3, 2):
        start = (lane_x * 4 + (y + dy) % 4) * 512 + sec * 256
        for half in range(2):
            source = wq_hbm.at[pl.ds(pl.multiple_of(start + half * 128, 128), 128)]
            links.send(source, wg.at[dy - 1, lane_x, sec, half], f_recv.at[dy - 1, half], {"tp": at(0, dy)})
    for half in range(2):
        xs.own_z(half)
    for dy in (1, 3, 2):
        links.send(kvps.at[(y + dy) % 4], kvpr.at[dy - 1], p_recv.at[dy - 1], {"tp": at(0, dy)})
    for half in range(2):
        ks.along_y(0, half)

    def weight(dy, dx, half):
        return wg.at[dy - 1, (lane_x - dx + 4) % 4, sec, half]

    def to_twin(dy, dx):
        part = wg.at[dy - 1, (lane_x - dx + 4) % 4, sec]
        links.send(part, part, w_recv.at[dy - 1, dx], twin)

    def weight_in(dy, dx, half):
        links.arrived(weight(dy, dx, half), g_recv.at[dy - 1, dx, half], twin)

    def fetched(dy):
        for half in range(2):
            part = weight(dy, 0, half)
            links.arrived(part, f_recv.at[dy - 1, half], twin)
            links.send(part, part, g_recv.at[dy - 1, 1, half], beside(1))
            links.send(part, part, g_recv.at[dy - 1, 3, half], beside(-1))
        to_twin(dy, 0)

    def near_x(dy):
        weight_in(dy, 1, 0)
        links.send(weight(dy, 1, 0), weight(dy, 1, 0), g_recv.at[dy - 1, 2, 0], beside(1))
        weight_in(dy, 3, 0)
        weight_in(dy, 3, 1)
        links.send(weight(dy, 3, 1), weight(dy, 3, 1), g_recv.at[dy - 1, 2, 1], beside(-1))
        to_twin(dy, 3)
        weight_in(dy, 1, 1)
        to_twin(dy, 1)

    def far_x(dy):
        weight_in(dy, 2, 0)
        weight_in(dy, 2, 1)
        to_twin(dy, 2)

    def from_twin(dy):
        for dx in range(4):
            part = wg.at[dy - 1, (lane_x - dx + 4) % 4, 1 - sec]
            links.arrived(part, w_recv.at[dy - 1, dx], twin)

    fetched(1)
    fetched(3)
    xs.arrived(1, 0, 0)
    xs.relay_z(0)
    xs.arrived(3, 0, 0)
    fetched(2)
    near_x(1)
    xs.arrived(3, 0, 1)
    xs.relay_z(1)
    xs.arrived(1, 0, 1)

    links.send(sk_hbm.at[:, head_cols(2)], relay.at[0], r_recv.at[0], {"tp": at(1, 0)})
    links.send(sv_hbm.at[:, head_cols(2)], relay.at[1], r_recv.at[1], {"tp": at(-1, 0)})
    for dz in (1, -1):
        ks.send(sk_hbm.at[:, head_cols(dz)], slot_of(dz % 4, 0), 0, dz, 0)
        ks.send(sv_hbm.at[:, head_cols(dz)], slot_of(dz % 4, 0), 1, dz, 0)

    near_x(3)

    for dy in range(1, 4):
        links.arrived(kvpr.at[dy - 1], p_recv.at[dy - 1], twin)
    for n in range(4):
        fresh = kvps[y, n].astype(F32)
        for dy in range(1, 4):
            fresh = fresh + kvpr[dy - 1, n].astype(F32)
        kvqs[n] = fresh
    near_x(2)
    far_x(1)
    far_x(3)
    for dz in range(1, 4):
        links.send(kvqs.at[(z + dz) % 4], kvqr.at[dz - 1], u_recv.at[dz - 1], {"tp": at(dz, 0)})
    ks.near_y(0)
    for half in range(2):
        xs.arrived(2, 0, half)

    def project(dy):
        total = 0.0
        for dz in range(4):
            from_z = (z - dz + 4) % 4
            weights = wl[from_z] if dy == 0 else wg[dy - 1, from_z].reshape(512, 2 * HD)
            total = total + dot(xg[dz].reshape(ROWS, -1), weights)
        return total

    for dy in (1, 3):
        from_twin(dy)
        qs[dy - 1] = project(dy)
        links.send(qs.at[dy - 1], qr.at[dy - 1], q_recv.at[dy - 1], {"tp": at(0, -dy)})
    for half in range(2):
        links.arrived(relay.at[half], r_recv.at[half], twin)
        ks.send(relay.at[half], slot_of(2, 0), half, 1 if half == 0 else -1, 0)
    far_x(2)
    from_twin(2)
    qs[1] = project(2)
    links.send(qs.at[1], qr.at[1], q_recv.at[1], {"tp": at(0, -2)})
    qacc[...] = project(0)

    for dz in (1, 3):
        for half in range(2):
            ks.arrived(dz, 0, half)
            ks.along_y(dz, half)
    for dz in range(1, 4):
        links.arrived(kvqr.at[dz - 1], u_recv.at[dz - 1], twin)
    fresh = kvqs[z] + kvqr[0] + kvqr[1] + kvqr[2]
    rows = pl.ds(pl.multiple_of(y * NODES, NODES), NODES)
    fresh_keys = rotate(fresh[:, :HD], cos_ref[rows, :], sin_ref[rows, :])
    nkv[0, y] = fresh_keys.astype(BF16)
    nkv[1, y] = fresh[:, HD:].astype(BF16)
    for half in range(2):
        ks.arrived(2, 0, half)
        ks.along_y(2, half)
    for dy in range(1, 4):
        links.send(nkv.at[:, y], nkv.at[:, y], n_recv.at[dy], {"tp": at(0, dy)})
    for dy in range(1, 4):
        links.arrived(qr.at[dy - 1], q_recv.at[dy - 1], twin)
    for head in range(2):
        cols = pl.ds(head * HD, HD)
        query = qacc[:, cols] + qr[0, :, cols] + qr[1, :, cols] + qr[2, :, cols]
        qh[head] = rotate(query, cos_ref[...], sin_ref[...]).astype(BF16)

    seq_wide = row // NODES

    def attend(pieces, first=False):
        def one_head(head, carry):
            queries = qh[head]
            scores = []
            for keys, _, visible in pieces:
                scores.append(jnp.where(visible(), dot(queries, keys(), ((1,), (1,))) * HD**-0.5, MASKED_SCORE))
            best = functools.reduce(jnp.maximum, scores)
            best = jnp.max(best, axis=1, keepdims=True)
            if not first:
                before = top_ref[head][:, :1]
                best = jnp.maximum(best, before)
                fade = jnp.exp(before - best)
            total = 0.0
            mix = 0.0
            for score, (_, values, _) in zip(scores, pieces):
                weights = jnp.exp(score - best)
                total = total + weights
                mix = mix + dot(weights.astype(BF16), values())
            total = jnp.sum(total, axis=1, keepdims=True)
            if not first:
                total = total + total_ref[head][:, :1] * fade
                mix = mix + mix_ref[head] * fade
            top_ref[head] = jnp.broadcast_to(best, (ROWS, HD))
            total_ref[head] = jnp.broadcast_to(total, (ROWS, HD))
            mix_ref[head] = mix
            return carry

        lax.fori_loop(0, 2, one_head, 0)

    def new_visible():
        reached = (closed[...].astype(F32) > 0.5).astype(jnp.int32)
        return sec * reached + (1 - sec) * (col <= row).astype(jnp.int32) > 0

    def tail_visible():
        return sec * (seq_wide == 0).astype(jnp.int32) > 0

    def stored(dz, dy):
        slot = slot_of(dz, dy)
        from_z, from_y = (z - dz + 4) % 4, (y - dy + 4) % 4

        def visible():
            in_prompt = prefix - (from_z * 4 + from_y) * ROWS
            in_cache = cache_ref[0, from_z] - from_y * ROWS
            mine = (seq_wide == from_z).astype(jnp.int32)
            return col < (1 - sec) * in_prompt + sec * in_cache * mine

        return (lambda: kg[slot], lambda: vg[slot], visible)

    ks.near_y(1)
    ks.near_y(3)
    for dy in range(1, 4):
        links.arrived(nkv.at[:, (y + 4 - dy) % 4], n_recv.at[dy], twin)
    links.send(nkv, tail, t_recv.at[0], twin)
    attend([(lambda: nkv[0].reshape(ROWS, HD), lambda: nkv[1].reshape(ROWS, HD), new_visible)], True)
    ks.near_y(2)
    attend([stored(dz, 0) for dz in range(4)])
    ks.far_y(0)
    attend([stored(0, 1), stored(0, 3), stored(0, 2)])
    attend([stored(1, 1), stored(1, 3), stored(3, 1), stored(3, 3)])
    links.arrived(tail, t_recv.at[0], twin)
    attend([(lambda: tail[0].reshape(ROWS, HD), lambda: tail[1].reshape(ROWS, HD), tail_visible)])
    ks.far_y(1)
    ks.far_y(3)
    attend([stored(2, 1), stored(2, 3), stored(1, 2), stored(3, 2)])
    ks.far_y(2)
    attend([stored(2, 2)])
    for head in range(2):
        done = (mix_ref[head] / total_ref[head]).astype(BF16)
        ag[0, :, :, head * HD : (head + 1) * HD] = done.reshape(2, ROWS // 2, HD)

    for half in range(2):
        ats.own_z(half)
        ats.along_y(0, half)

    def finish(dz, dy, first=False):
        source = pl.multiple_of(at(-dz, -dy) * 256, 256)
        part = dot(ag[slot_of(dz, dy)].reshape(ROWS, -1), wo[pl.ds(source, 256), :])
        oacc[...] = part if first else oacc[...] + part

    finish(0, 0, True)
    ats.near_y(0)
    ats.arrived(1, 0, 0)
    ats.relay_z(0)
    ats.along_y(1, 0)
    ats.arrived(3, 0, 0)
    ats.along_y(3, 0)
    ats.arrived(3, 0, 1)
    ats.relay_z(1)
    ats.along_y(3, 1)
    ats.arrived(1, 0, 1)
    ats.along_y(1, 1)
    finish(0, 1)
    finish(0, 3)
    finish(1, 0)
    finish(3, 0)
    ats.far_y(0)
    finish(0, 2)
    for half in range(2):
        ats.arrived(2, 0, half)
        ats.along_y(2, half)
    ats.near_y(1)
    ats.near_y(3)
    finish(2, 0)
    finish(1, 1)
    finish(1, 3)
    finish(3, 1)
    finish(3, 3)
    ats.near_y(2)
    finish(2, 1)
    finish(2, 3)
    ats.far_y(1)
    finish(1, 2)
    ats.far_y(3)
    finish(3, 2)
    ats.far_y(2)
    finish(2, 2)
    out_ref[...] = oacc[...].astype(BF16)
    links.finish()


def per_device(
    states, q_weight, kv_weight, o_weight, store_keys, store_values, prefix_len, cache_len, parents
):
    exponent = np.arange(HD, dtype=np.float32) % (HD // 2) * np.float32(-2.0 / HD)
    frequency = np.exp(exponent * np.log(np.float32(ROPE_BASE))).astype(np.float32)
    x = states[0, 0].reshape(2, ROWS // 2, -1)
    any_space = pl.BlockSpec(memory_space=pl.ANY)
    in_vmem = pl.BlockSpec(memory_space=pltpu.VMEM)
    in_smem = pl.BlockSpec(memory_space=pltpu.SMEM)
    dma = pltpu.SemaphoreType.DMA
    out = pl.pallas_call(
        kernel,
        out_shape=jax.ShapeDtypeStruct((ROWS, o_weight.shape[1]), BF16),
        in_specs=[in_smem, in_smem, in_vmem, in_vmem] + [any_space] * 6,
        out_specs=in_vmem,
        scratch_shapes=[
            pltpu.VMEM((4, 2, ROWS // 2, 512), BF16),
            pltpu.VMEM((4, 512, 2 * HD), BF16),
            pltpu.VMEM((3, 4, 2, 2, 128, 2 * HD), BF16),
            pltpu.VMEM(kv_weight.shape, BF16),
            pltpu.VMEM(o_weight.shape, BF16),
            pltpu.VMEM((4, 4, NODES, 2 * HD), BF16),
            pltpu.VMEM((3, 4, NODES, 2 * HD), BF16),
            pltpu.VMEM((4, NODES, 2 * HD), F32),
            pltpu.VMEM((3, NODES, 2 * HD), F32),
            pltpu.VMEM((16, ROWS, HD), BF16),
            pltpu.VMEM((16, ROWS, HD), BF16),
            pltpu.VMEM((2, ROWS, HD), BF16),
            pltpu.VMEM((2, 4, NODES, HD), BF16),
            pltpu.VMEM((2, 4, NODES, HD), BF16),
            pltpu.VMEM((ROWS, 2 * HD), F32),
            pltpu.VMEM((3, ROWS, 2 * HD), F32),
            pltpu.VMEM((3, ROWS, 2 * HD), F32),
            pltpu.VMEM((2, ROWS, HD), BF16),
            pltpu.VMEM((ROWS, ROWS), BF16),
            pltpu.VMEM((ROWS, HD), F32),
            pltpu.VMEM((ROWS, HD), F32),
            pltpu.VMEM((2, ROWS, HD), F32),
            pltpu.VMEM((2, ROWS, HD), F32),
            pltpu.VMEM((2, ROWS, HD), F32),
            pltpu.VMEM((16, 2, ROWS // 2, 2 * HD), BF16),
            pltpu.VMEM((ROWS, o_weight.shape[1]), F32),
            dma((9,)),
            dma((144,)),
            dma((4, 2)),
            dma((16, 2)),
            dma((2,)),
            dma((3,)),
            dma((3,)),
            dma((4,)),
            dma((1,)),
            dma((16, 2)),
            dma((3, 2)),
            dma((3, 4, 2)),
            dma((3, 4)),
            dma((3,)),
        ],
        compiler_params=pltpu.CompilerParams(
            collective_id=0, has_side_effects=True, vmem_limit_bytes=56 * 2**20
        ),
    )(
        prefix_len, cache_len, parents[0], jnp.asarray(frequency)[None], x, q_weight, kv_weight, o_weight,
        store_keys[0, 0], store_values[0, 0],
    )
    return out[None, None]


def solution(mesh):
    return jax.shard_map(
        per_device,
        mesh=mesh,
        in_specs=(
            P("section", "rep", None, "tp"),
            P(None, "tp"),
            P("tp", None),
            P(None, "tp"),
            P("section", "rep", "tp", None),
            P("section", "rep", "tp", None),
            P(),
            P("rep", None),
            P("rep", None, None),
        ),
        out_specs=P("section", "rep", None, "tp"),
        check_vma=False,
    )
```
